32 devices in a mesh: seq: 2 (over x), fsdp: 16 (over z, y, core).
Axes of the slice: x: 2, y: 2, z: 4, core: 2. Of those that a mesh axis runs over, the one named last changes fastest.
Arguments:
- inputs: bfloat16 [16, 256, 2560], P('fsdp', 'seq'), may hold values from -6 to 6
- step_sizes: float32 [16, 256, 40], P('fsdp', 'seq'), may hold values from 0 to 1.6
- input_map: bfloat16 [16, 256, 128], P('fsdp', 'seq'), may hold values from -6 to 6
- output_map: bfloat16 [16, 256, 128], P('fsdp', 'seq'), may hold values from -6 to 6
- decay_rate: float32 [40], replicated, may hold values from 0.5 to 2
- skip_gain: float32 [40], replicated, may hold values from 0.5 to 1.5
- norm_gain: float32 [2560], replicated, may hold values from 0.1 to 1.9
- query_weight: bfloat16 [2560, 1024], P('fsdp', 'seq'), may hold values from -1 to 1
- key_weight: bfloat16 [2560, 1024], P('fsdp', 'seq'), may hold values from -1 to 1
- value_weight: bfloat16 [2560, 1024], P('fsdp', 'seq'), may hold values from -0.125 to 0.125
- cotangent: bfloat16 [16, 256, 1024], P('fsdp', 'seq'), may hold values from -6 to 6
Outputs:
- attended: bfloat16 [16, 256, 1024], P('fsdp', 'seq')
- grad_query: float32 [2560, 1024], P('fsdp', 'seq')
- grad_key: float32 [2560, 1024], P('fsdp', 'seq')
- grad_value: float32 [2560, 1024], P('fsdp', 'seq')
The draws below stay inside these ranges and needn't reach their ends.
All inputs are finite; a program needn't handle non-finite values.
Results may differ from the reference program's by a relative error of at most 0.01505.
The reference program's roundings to bfloat16 on the way count: a program that leaves them out, or rounds other values in their place, can miss the bound.
Values may be sent and summed in bfloat16 or wider, within the bound.
No kernel may reach another device: no remote copies, remote signals or barrier semaphores. Data moves between devices by JAX's collectives and lax.ppermute only.
A program may use at most 64 MiB of HBM per device.

```python
import math
from functools import partial
import jax
import jax.numpy as jnp
from jax import lax

GROUP = 128
SSM_HEADS = 40
SSM_DIM = 64
STATE = 128
ATT_HEADS = 16
ATT_DIM = 64
FEAT = 2560
COLS = 1024
SEQUENCE_LENGTH = 256
SEQUENCE_COUNT = 16


def draw_step_sizes(key, part):
    root_random_key, noise_random_key, spike_random_key = jax.random.split(key, 3)
    lowest = math.log(0.2 / SEQUENCE_LENGTH)
    highest = math.log(0.05)
    level_values = jnp.exp(jax.random.uniform(root_random_key, (SEQUENCE_COUNT, 1, SSM_HEADS), jnp.float32, lowest, highest))
    noise_amplitude = jax.random.uniform(noise_random_key, (SEQUENCE_COUNT, SEQUENCE_LENGTH, SSM_HEADS), jnp.float32, 0.5, 2.0)
    spike_positions = jax.random.randint(spike_random_key, (SEQUENCE_COUNT, 4), 0, SEQUENCE_LENGTH)
    spike_values = jnp.sum((jnp.arange(SEQUENCE_LENGTH)[None, :, None] == spike_positions[:, None, :]).astype(jnp.float32), axis=2)
    return level_values * noise_amplitude + 0.35 * spike_values[:, :, None]


def projection_pair(key):
    first_key = jax.random.fold_in(key, 101)
    second_key = jax.random.fold_in(key, 102)
    scale = FEAT ** (-0.5)
    first = jnp.clip(jax.random.normal(first_key, (FEAT, COLS), jnp.float32), -4.0, 4.0) * scale
    second = jnp.clip(jax.random.normal(second_key, (FEAT, COLS), jnp.float32), -4.0, 4.0) * scale
    return (first, second)


def draw_query_weight(key, part):
    return projection_pair(key)[0].astype(jnp.bfloat16)


def draw_key_weight(key, part):
    return projection_pair(key)[1].astype(jnp.bfloat16)


def block_scale(own_key, extent, shards, low, high):
    gain, own = 1.0, jax.random.fold_in(own_key, 6)
    for axis_at, blocks in shards:
        heights = jnp.exp(jax.random.uniform(jax.random.fold_in(own, axis_at), (blocks,), jnp.float32, low / len(shards), high / len(shards)))
        gain = gain * jnp.repeat(heights, extent[axis_at] // blocks).reshape([-1 if axis == axis_at else 1 for axis in range(len(extent))])
    return gain


def centred(own_key, dims, scale, bound, cuts=(), dtype=jnp.bfloat16):
    gain = block_scale(own_key, dims, cuts, -0.22, 0.18) if cuts else 1.0
    entries = jax.random.normal(own_key, dims, jnp.float32) * scale * gain
    return jnp.minimum(jnp.maximum(entries, -bound), bound).astype(dtype)


def setup_inputs(seed: int = 0) -> dict:
    streams_of = jax.random.split(jax.random.key(seed), 12)
    return {
        "inputs": centred(streams_of[0], (SEQUENCE_COUNT, SEQUENCE_LENGTH, FEAT), 1.0, 6.0, ((0, 16), (1, 2))),
        "step_sizes": draw_step_sizes(jax.random.fold_in(streams_of[11], 71), 0),
        "input_map": centred(streams_of[2], (SEQUENCE_COUNT, SEQUENCE_LENGTH, STATE), 1.0, 6.0, ((0, 16), (1, 2))),
        "output_map": centred(streams_of[3], (SEQUENCE_COUNT, SEQUENCE_LENGTH, STATE), 1.0, 6.0, ((0, 16), (1, 2))),
        "decay_rate": jnp.clip(jnp.exp(jax.random.uniform(streams_of[4], (SSM_HEADS,), jnp.float32, math.log(0.5), math.log(2.0))), 0.5, 2.0),
        "skip_gain": jnp.clip(jax.random.uniform(streams_of[5], (SSM_HEADS,), jnp.float32, 0.5, 1.5), 0.5, 1.5),
        "norm_gain": jnp.clip(1.0 + 0.18 * jax.random.normal(streams_of[6], (FEAT,), jnp.float32), 0.1, 1.9),
        "query_weight": draw_query_weight(jax.random.fold_in(streams_of[11], 71), 0),
        "key_weight": draw_key_weight(jax.random.fold_in(streams_of[11], 71), 0),
        "value_weight": centred(streams_of[9], (FEAT, COLS), FEAT ** -0.5, 0.125, ((0, 16), (1, 2))),
        "cotangent": centred(streams_of[10], (SEQUENCE_COUNT, SEQUENCE_LENGTH, COLS), 1.0, 6.0, ((0, 16), (1, 2))),
    }


precise = lax.Precision.HIGHEST
epsilon = 1e-05
very_low = -1e+30

def mixer_block(carried, portion, decay_rate):
    head_inputs, block_steps, block_in_map, block_out_map = portion
    block_len = block_steps.shape[0]
    running = jnp.cumsum(-block_steps * decay_rate[None, :], axis=0)
    positions = jnp.arange(block_len)
    causal = (positions[:, None] >= positions[None, :])[None]
    spread = running.T[:, :, None] - running.T[:, None, :]
    decays = jnp.where(causal, jnp.exp(jnp.where(causal, spread, 0.0)), 0.0)
    intersection = jnp.dot(block_out_map, block_in_map.T, preferred_element_type=jnp.float32)
    mixing = decays * intersection[None] * block_steps.T[:, None, :]
    within = jnp.einsum('hij,jhp->ihp', mixing, head_inputs, precision=precise)
    readout = jnp.einsum('in,hpn->ihp', block_out_map.astype(jnp.float32), carried, precision=precise)
    within = within + readout * jnp.exp(running)[:, :, None]
    remaining = jnp.exp(running[-1][None, :] - running) * block_steps
    written = jnp.einsum('jh,jhp,jn->hpn', remaining, head_inputs, block_in_map.astype(jnp.float32), precision=precise)
    carried = carried * jnp.exp(running[-1])[:, None, None] + written
    return (carried, within)

def mixer_segment(seq_inputs, seq_steps, seq_in_map, seq_out_map, decay_rate, carried):
    tokens_here = seq_inputs.shape[0]
    blocks_here = tokens_here // GROUP
    heads_here = decay_rate.shape[0]
    head_inputs = seq_inputs.astype(jnp.float32).reshape(blocks_here, GROUP, heads_here, -1)
    portions = (head_inputs, seq_steps.reshape(blocks_here, GROUP, heads_here), seq_in_map.reshape(blocks_here, GROUP, -1), seq_out_map.reshape(blocks_here, GROUP, -1))
    carried, outputs = lax.scan(partial(mixer_block, decay_rate=decay_rate), carried, portions)
    return (carried, outputs.reshape(tokens_here, heads_here, -1))

def normalize(mixed_out, seq_inputs, skip_gain, norm_gain):
    combined = mixed_out + skip_gain[None, :, None] * seq_inputs.astype(jnp.float32).reshape(mixed_out.shape)
    flattened = combined.reshape(mixed_out.shape[0], -1)
    mean_square = lax.optimization_barrier(jnp.mean(flattened * flattened, axis=1, keepdims=True))
    return (flattened * lax.rsqrt(mean_square + epsilon) * norm_gain[None, :]).astype(jnp.bfloat16)

def one_head(portion):
    query_rows, key_rows, value_rows, grad_rows = portion
    length_here = query_rows.shape[0]
    factor = 1.0 / math.sqrt(query_rows.shape[1])
    scores = jnp.dot(query_rows, key_rows.T, preferred_element_type=jnp.float32) * factor
    positions = jnp.arange(length_here)
    allowed = positions[None, :] <= positions[:, None]
    scores = jnp.where(allowed, scores, very_low)
    highest = lax.optimization_barrier(jnp.max(scores, axis=1, keepdims=True))
    weights = jnp.where(allowed, jnp.exp(scores - highest), 0.0)
    probability = weights / lax.optimization_barrier(jnp.sum(weights, axis=1, keepdims=True))
    rounded = probability.astype(jnp.bfloat16)
    attended = jnp.dot(rounded, value_rows, preferred_element_type=jnp.float32).astype(jnp.bfloat16)
    value_grad = jnp.dot(rounded.T, grad_rows, preferred_element_type=jnp.float32)
    prob_grad = jnp.dot(grad_rows, value_rows.T, preferred_element_type=jnp.float32)
    centered = lax.optimization_barrier(jnp.sum(probability * prob_grad, axis=1, keepdims=True))
    score_grad = (probability * (prob_grad - centered) * factor).astype(jnp.bfloat16)
    query_grad = jnp.dot(score_grad, key_rows, preferred_element_type=jnp.float32)
    key_grad = jnp.dot(score_grad.T, query_rows, preferred_element_type=jnp.float32)
    return (attended, query_grad.astype(jnp.bfloat16), key_grad.astype(jnp.bfloat16), value_grad.astype(jnp.bfloat16))

def reference(inputs, step_sizes, input_map, output_map, decay_rate, skip_gain, norm_gain, query_weight, key_weight, value_weight, cotangent):
    columns = query_weight.shape[1]
    joined = jnp.concatenate([query_weight, key_weight, value_weight], axis=1)
    empty_state = jnp.zeros((SSM_HEADS, SSM_DIM, STATE), jnp.float32)

    def by_heads(matrix):
        return matrix.reshape(SEQUENCE_LENGTH, ATT_HEADS, ATT_DIM).transpose(1, 0, 2)

    def by_columns(matrix):
        return matrix.transpose(1, 0, 2).reshape(SEQUENCE_LENGTH, columns)

    def one_sequence(accumulated, portion):
        seq_inputs, seq_steps, seq_in_map, seq_out_map, seq_grad = portion
        _, mixed_out = mixer_segment(seq_inputs, seq_steps, seq_in_map, seq_out_map, decay_rate, empty_state)
        normed = normalize(mixed_out, seq_inputs, skip_gain, norm_gain)
        projected = jnp.dot(normed, joined, preferred_element_type=jnp.float32).astype(jnp.bfloat16)
        results = lax.map(one_head, (by_heads(projected[:, :columns]), by_heads(projected[:, columns:2 * columns]), by_heads(projected[:, 2 * columns:]), by_heads(seq_grad)))
        attended = by_columns(results[0])
        gradients = jnp.concatenate([by_columns(results[1]), by_columns(results[2]), by_columns(results[3])], axis=1)
        accumulated = accumulated + jnp.dot(normed.T, gradients, preferred_element_type=jnp.float32)
        return (accumulated, attended)
    initial = jnp.zeros((FEAT, 3 * columns), jnp.float32)
    summed, attended = lax.scan(one_sequence, initial, (inputs, step_sizes, input_map, output_map, cotangent))
    return (attended, summed[:, :columns], summed[:, columns:2 * columns], summed[:, 2 * columns:])
```

```python
import math

import jax
import jax.numpy as jnp
from jax import lax
from jax.experimental import pallas as pl
from jax.experimental.pallas import tpu as pltpu
from jax.sharding import Mesh, PartitionSpec as P

GROUP = 128
LANES = 128
ATT_DIM = 64
EPSILON = 1e-05
VERY_LOW = -1e30


def split_two(value):
    upper = value.astype(jnp.bfloat16)
    lower = (value - upper.astype(jnp.float32)).astype(jnp.bfloat16)
    return upper, lower


def matmul(left, right):
    return jnp.dot(left, right, preferred_element_type=jnp.float32)


def matmul_nt(left, right):
    return lax.dot_general(
        left, right, (((1,), (1,)), ((), ())), preferred_element_type=jnp.float32
    )


def matmul_tn(left, right):
    return lax.dot_general(
        left, right, (((0,), (0,)), ((), ())), preferred_element_type=jnp.float32
    )


def mixer_kernel(
    place, block, steps_in, rate, skip, gain, normed, state, mixed, *, features, blocks
):
    at = pl.program_id(0)
    steps = steps_in[0]
    rows = lax.broadcasted_iota(jnp.int32, (GROUP, GROUP), 0)
    columns = lax.broadcasted_iota(jnp.int32, (GROUP, GROUP), 1)
    causal = rows >= columns
    running = jnp.dot(
        causal.astype(jnp.float32),
        -steps * rate[...],
        precision=lax.Precision.HIGHEST,
        preferred_element_type=jnp.float32,
    )
    running_t = running.T
    steps_t = steps.T
    in_map = block[0, :, features : features + LANES]
    out_map = block[0, :, features + LANES : features + 2 * LANES]
    meeting = jnp.where(causal, matmul_nt(out_map, in_map), 0.0)
    first = lax.broadcasted_iota(jnp.int32, (GROUP, LANES), 1) < LANES // 2
    first_16 = first.astype(jnp.float32).astype(jnp.bfloat16)
    second_16 = 1 - first_16
    tiles = features // LANES

    def widen(table, tile):
        shape = (table.shape[0], LANES)
        return jnp.where(
            first[: table.shape[0]],
            jnp.broadcast_to(table[:, 2 * tile : 2 * tile + 1], shape),
            jnp.broadcast_to(table[:, 2 * tile + 1 : 2 * tile + 2], shape),
        )

    for tile in range(tiles):
        here = slice(tile * LANES, (tile + 1) * LANES)
        own = block[0, :, here]
        uppers, lowers = [], []
        for head in (2 * tile, 2 * tile + 1):
            spread = running[:, head : head + 1] - running_t[head : head + 1, :]
            decays = jnp.exp(jnp.where(causal, spread, VERY_LOW))
            upper, lower = split_two(decays * (meeting * steps_t[head : head + 1, :]))
            uppers.append(upper)
            lowers.append(lower)
        apart = jnp.concatenate([own * first_16, own * second_16], axis=0)
        within = matmul(jnp.concatenate(uppers, axis=1), apart) + matmul(
            jnp.concatenate(lowers, axis=1), apart
        )
        mixed[:, here] = within + skip[:, here] * own.astype(jnp.float32)

    if blocks > 1:

        @pl.when(at > 0)
        def _():
            grown = jnp.exp(running)
            for tile in range(tiles):
                here = slice(tile * LANES, (tile + 1) * LANES)
                upper, lower = split_two(state[:, here])
                readout = matmul(out_map, upper) + matmul(out_map, lower)
                mixed[:, here] = mixed[:, here] + readout * widen(grown, tile)

        @pl.when(at < blocks - 1)
        def _():
            last = running[GROUP - 1 : GROUP, :]
            remaining = jnp.exp(last - running) * steps
            kept = jnp.exp(last)
            in_map_t = in_map.astype(jnp.float32).T.astype(jnp.bfloat16)
            for tile in range(tiles):
                here = slice(tile * LANES, (tile + 1) * LANES)
                upper, lower = split_two(
                    widen(remaining, tile) * block[0, :, here].astype(jnp.float32)
                )
                written = matmul(in_map_t, upper) + matmul(in_map_t, lower)
                earlier = jnp.where(at > 0, state[:, here] * widen(kept, tile), 0.0)
                state[:, here] = earlier + written

    total = jnp.zeros((GROUP, LANES), jnp.float32)
    for tile in range(tiles):
        part = mixed[:, tile * LANES : (tile + 1) * LANES]
        total = total + part * part
    mean_square = jnp.sum(total, axis=1, keepdims=True) * (1.0 / features)
    scale = lax.rsqrt(mean_square + EPSILON)
    for tile in range(tiles):
        here = slice(tile * LANES, (tile + 1) * LANES)
        normed[:, here] = (mixed[:, here] * scale * gain[:, here]).astype(jnp.bfloat16)


def mix(place, blocks_in, steps_in, rate, skip, gain):
    blocks, _, width = blocks_in.shape
    features = gain.shape[1]

    def slot(at, place):
        return (lax.rem(place[0] - at + blocks, blocks), 0, 0)

    def same(at, place):
        return (0, 0)

    return pl.pallas_call(
        lambda *refs: mixer_kernel(*refs, features=features, blocks=blocks),
        grid_spec=pltpu.PrefetchScalarGridSpec(
            num_scalar_prefetch=1,
            grid=(blocks,),
            in_specs=[
                pl.BlockSpec((1, GROUP, width), slot),
                pl.BlockSpec((1, GROUP, LANES), slot),
                pl.BlockSpec((1, LANES), same),
                pl.BlockSpec((1, features), same),
                pl.BlockSpec((1, features), same),
            ],
            out_specs=pl.BlockSpec((GROUP, features), lambda at, place: (at, 0)),
            scratch_shapes=[
                pltpu.VMEM((LANES, features), jnp.float32),
                pltpu.VMEM((GROUP, features), jnp.float32),
            ],
        ),
        out_shape=jax.ShapeDtypeStruct((blocks * GROUP, features), jnp.bfloat16),
        compiler_params=pltpu.CompilerParams(dimension_semantics=("arbitrary",)),
        name="mixer",
    )(place, blocks_in, steps_in, rate, skip, gain)


def attend_kernel(order, projected, cotangent, attended, gradients):
    length = projected.shape[0]
    factor = 1.0 / math.sqrt(ATT_DIM)
    query = projected[:, :LANES]
    key = projected[:, LANES : 2 * LANES]
    value = projected[:, 2 * LANES :]
    arriving = cotangent[...].reshape(length, LANES)
    lane = lax.broadcasted_iota(jnp.int32, (length, LANES), 1)
    allowed = lax.broadcasted_iota(jnp.int32, (length, length), 1) <= lax.broadcasted_iota(
        jnp.int32, (length, length), 0
    )
    results = []
    for head in range(LANES // ATT_DIM):
        mine_32 = (lane // ATT_DIM == head).astype(jnp.float32)
        mine = mine_32.astype(jnp.bfloat16)
        scores = matmul_nt(query * mine, key) * factor
        scores = jnp.where(allowed, scores, VERY_LOW)
        weights = jnp.exp(scores - jnp.max(scores, axis=1, keepdims=True))
        weights = jnp.where(allowed, weights, 0.0)
        probability = weights / jnp.sum(weights, axis=1, keepdims=True)
        rounded = probability.astype(jnp.bfloat16)
        prob_grad = matmul_nt(arriving * mine, value)
        centered = jnp.sum(probability * prob_grad, axis=1, keepdims=True)
        score_grad = (probability * (prob_grad - centered) * factor).astype(jnp.bfloat16)
        results.append(
            [
                part * mine_32
                for part in (
                    matmul(rounded, value),
                    matmul(score_grad, key),
                    matmul_tn(score_grad, query),
                    matmul_tn(rounded, arriving),
                )
            ]
        )
    joined = [sum(parts[1:], parts[0]).astype(jnp.bfloat16) for parts in zip(*results)]
    attended[...] = joined[0].reshape(attended.shape)
    for at in range(3):
        gradients[:, at * LANES : (at + 1) * LANES] = joined[at + 1]


def attend(order, projected, cotangent):
    blocks, sequences, group, _ = cotangent.shape
    length = blocks * group

    def rows(at, order):
        return (at, 0)

    def picked(at, order):
        return (0, order[at], 0, 0)

    return pl.pallas_call(
        attend_kernel,
        grid_spec=pltpu.PrefetchScalarGridSpec(
            num_scalar_prefetch=1,
            grid=(sequences,),
            in_specs=[
                pl.BlockSpec((length, 3 * LANES), rows),
                pl.BlockSpec((blocks, 1, group, LANES), picked),
            ],
            out_specs=[
                pl.BlockSpec((blocks, 1, group, LANES), picked),
                pl.BlockSpec((length, 3 * LANES), rows),
            ],
        ),
        out_shape=[
            jax.ShapeDtypeStruct(cotangent.shape, jnp.bfloat16),
            jax.ShapeDtypeStruct(projected.shape, jnp.bfloat16),
        ],
        compiler_params=pltpu.CompilerParams(dimension_semantics=("arbitrary",)),
        name="attend",
    )(order, projected, cotangent)


def shifted(value, names, sizes, shift):
    count = math.prod(sizes)

    def target(index):
        moved, scale = 0, 1
        for size, step in zip(reversed(sizes), reversed(shift)):
            moved += (index % size + step) % size * scale
            index, scale = index // size, scale * size
        return moved

    return lax.ppermute(value, names, [(index, target(index)) for index in range(count)])


def body(sizes, inputs, step_sizes, input_map, output_map, decay_rate, skip_gain, norm_gain,
         query_weight, key_weight, value_weight, cotangent):
    n_seq, n_out, n_a, n_b = sizes
    place = lax.axis_index("seq")
    at_out, at_a, at_b = (lax.axis_index(name) for name in ("out", "a", "b"))
    features = inputs.shape[2]
    mixer_heads = decay_rate.shape[0]
    sharing = n_a * n_b

    weights = jnp.stack([query_weight, key_weight, value_weight], axis=1)
    rows_here = weights.shape[0]
    weights = weights.reshape(rows_here, 3, sharing, LANES).transpose(2, 0, 1, 3)
    weights = weights.reshape(sharing, rows_here, 3 * LANES)
    if sharing > 1:
        weights = lax.all_to_all(weights, ("a", "b"), split_axis=0, concat_axis=0, tiled=True)
    weights = weights.reshape(sharing * rows_here, 3 * LANES)
    if n_out <= 8:
        own, whole = weights, jnp.zeros((n_out,) + weights.shape, weights.dtype)
        for step in range(n_out):
            piece = own if step == 0 else shifted(own, ("out",), (n_out,), (step,))
            whole = lax.dynamic_update_index_in_dim(
                whole, piece, lax.rem(at_out - step + n_out, n_out), 0
            )
    else:
        whole = lax.all_gather(weights, "out", axis=0)
    whole = whole.reshape(n_out * sharing * rows_here, 3 * LANES)

    arriving = cotangent[0].reshape(GROUP, n_seq * sharing, LANES).transpose(1, 0, 2)
    arriving = lax.all_to_all(arriving, ("seq", "a", "b"), split_axis=0, concat_axis=0, tiled=True)
    arriving = arriving.reshape(n_seq, sharing, GROUP, LANES)

    bundle = jnp.concatenate([inputs[0], input_map[0], output_map[0]], axis=1)
    steps = step_sizes[0]
    rate = jnp.pad(decay_rate, (0, LANES - mixer_heads))[None]
    skip = jnp.repeat(skip_gain, features // mixer_heads)[None]
    gain = norm_gain[None]
    normed = []
    for step_a in range(n_a):
        parts = []
        for step_s in range(n_seq):
            moved = (bundle, steps)
            if step_a or step_s:
                moved = tuple(
                    shifted(part, ("seq", "a"), (n_seq, n_a), (step_s, step_a)) for part in moved
                )
            parts.append(moved)
        blocks_in = jnp.stack([part[0] for part in parts])
        steps_in = jnp.pad(
            jnp.stack([part[1] for part in parts]), ((0, 0), (0, 0), (0, LANES - mixer_heads))
        )
        own = mix(place[None], blocks_in, steps_in, rate, skip, gain)
        for step_b in range(n_b):
            piece = own if step_b == 0 else shifted(own, ("b",), (n_b,), (step_b,))
            source = lax.rem(at_a - step_a + n_a, n_a) * n_b + lax.rem(at_b - step_b + n_b, n_b)
            normed.append((source, piece))
    order = jnp.stack([source for source, _ in normed]).astype(jnp.int32)
    normed = jnp.concatenate([piece for _, piece in normed], axis=0)

    projected = matmul(normed, whole).astype(jnp.bfloat16)
    attended, gradients = attend(order, projected, arriving)

    shares = matmul_tn(normed, gradients).astype(jnp.bfloat16)
    shares = shares.reshape(n_out * sharing, rows_here, 3 * LANES)
    shares = lax.all_to_all(shares, ("out", "a", "b"), split_axis=0, concat_axis=0, tiled=True)
    shares = shares.reshape(n_out, sharing, rows_here, 3 * LANES).astype(jnp.float32)
    summed = jnp.sum(shares, axis=0).reshape(sharing, rows_here, 3, LANES)
    summed = summed.transpose(2, 1, 0, 3).reshape(3, rows_here, sharing * LANES)

    attended = attended.reshape(n_seq * sharing, GROUP, LANES)
    attended = lax.all_to_all(attended, ("seq", "a", "b"), split_axis=0, concat_axis=0, tiled=True)
    attended = attended.transpose(1, 0, 2).reshape(1, GROUP, n_seq * sharing * LANES)
    return attended, summed[0], summed[1], summed[2]


def solution(mesh):
    n_seq, n_fsdp = mesh.shape["seq"], mesh.shape["fsdp"]

    def step(*arguments):
        columns = arguments[7].shape[1]
        sharing = columns // LANES // n_seq
        n_b = 2 if sharing % 2 == 0 else 1
        sizes = (n_seq, n_fsdp // sharing, sharing // n_b, n_b)
        finer = Mesh(mesh.devices.reshape(sizes), ("seq", "out", "a", "b"))
        rows = ("out", "a", "b")
        tokens = P(rows, "seq", None)
        weight = P(rows, "seq")
        return jax.shard_map(
            lambda *local: body(sizes, *local),
            mesh=finer,
            in_specs=(tokens,) * 4 + (P(),) * 3 + (weight,) * 3 + (tokens,),
            out_specs=(tokens, weight, weight, weight),
            check_vma=False,
        )(*arguments)

    return step
```
